32 devices in a mesh: rep: 32 (over z, y, x, core).
Axes of the slice: x: 2, y: 2, z: 4, core: 2. Of those that a mesh axis runs over, the one named last changes fastest.
Arguments:
- inputs: bfloat16 [16384, 1024], P('rep'), may hold values from -6 to 6
- out_grads: bfloat16 [16384, 4096], P('rep'), may hold values from -0.29882812 to 0.29882812
- error_in: bfloat16 [32, 1024, 4096], P('rep'), may hold values from -6 to 6
- q_start: float32 [32, 4096], replicated, may hold values from -0.09375 to 0.09375
- master: float32 [1024, 4096], P(None, 'rep'), may hold values from -1.2 to 1.2
Outputs:
- error_out: bfloat16 [32, 1024, 4096], P('rep')
- q_out: float32 [32, 4096], replicated
- master_out: float32 [1024, 4096], P(None, 'rep')
The draws below stay inside these ranges and needn't reach their ends.
All inputs are finite; a program needn't handle non-finite values.
Results may differ from the reference program's by a relative error of at most 0.001.
Values sent between devices are 32-bit elements; how exact they have to be, the bound alone decides.
No kernel may reach another device: no remote copies, remote signals or barrier semaphores. Data moves between devices by JAX's collectives and lax.ppermute only.
A program may use at most 128 MiB of HBM per device.

```python
import jax
import jax.numpy as jnp
from jax import lax

D = 1024
FF = 4096
RANK = 32
ITERS = 3
TOKENS = 16384
N_REP = 32


def steps_of(rng, shape, pieces, low, top_value):
    gain, own = 1.0, jax.random.fold_in(rng, 6)
    for position, parts in pieces:
        heights = jnp.exp(jax.random.uniform(jax.random.fold_in(own, position), (parts,), jnp.float32, low / len(pieces), top_value / len(pieces)))
        gain = gain * jnp.repeat(heights, shape[position] // parts).reshape([-1 if axis == position else 1 for axis in range(len(shape))])
    return gain


def gaussian(own_key, extent, spread, limit, pieces=(), held_as=jnp.bfloat16):
    result = jax.random.normal(own_key, extent, jnp.float32) * spread
    if len(pieces) > 0:
        result = steps_of(own_key, extent, pieces, -0.22, 0.18) * result
    return jnp.clip(result, min=-limit, max=limit).astype(held_as)


def setup_inputs(seed: int = 0) -> dict:
    splits = jax.random.split(jax.random.key(seed), 6)
    return {
        "inputs": gaussian(splits[0], (TOKENS, D), 1.0, 6.0, ((0, 32),)),
        "out_grads": gaussian(splits[1], (TOKENS, FF), 0.045, 0.29882812, ((0, 32),)),
        "error_in": gaussian(splits[2], (N_REP, D, FF), 1.0, 6.0, ((0, 32),)),
        "q_start": gaussian(splits[3], (RANK, FF), FF ** -0.5, 0.09375, (), jnp.float32),
        "master": gaussian(splits[4], (D, FF), 0.2, 1.2, ((1, 32),), jnp.float32),
    }


def orthonormal(rows):
    basis = jnp.zeros_like(rows)
    for k in range(rows.shape[0]):
        vector = rows[k]
        coef = jnp.dot(basis, vector, precision=lax.Precision.HIGHEST)
        vector = vector - jnp.dot(coef, basis, precision=lax.Precision.HIGHEST)
        basis = basis.at[k].set(vector / jnp.sqrt(jnp.sum(vector * vector) + 1.0))
    return basis

def reference(inputs, out_grads, error_in, q_start, master):
    tok = inputs.shape[0] // N_REP
    xs = inputs.reshape(N_REP, tok, inputs.shape[1])
    dys = out_grads.reshape(N_REP, tok, out_grads.shape[1])

    def one_replica(items):
        x_rows, dy_rows, error = items
        grad = lax.dot_general(x_rows, dy_rows, (((0,), (0,)), ((), ())), preferred_element_type=jnp.float32)
        return grad + error.astype(jnp.float32)
    merged = lax.map(one_replica, (xs, dys, error_in))
    merged_sum = lax.optimization_barrier(jnp.sum(merged, axis=0))
    factor = q_start
    basis = None
    for step in range(ITERS):
        p_total = lax.dot_general(factor, merged_sum, (((1,), (1,)), ((), ())), precision=lax.Precision.HIGHEST, preferred_element_type=jnp.float32)
        basis = orthonormal(p_total)
        factor = jnp.dot(basis, merged_sum, precision=lax.Precision.HIGHEST, preferred_element_type=jnp.float32) / N_REP
    recon = lax.dot_general(basis, factor, (((0,), (0,)), ((), ())), precision=lax.Precision.HIGHEST, preferred_element_type=jnp.float32)
    error_out = (merged - recon[None]).astype(jnp.bfloat16)
    master_out = master - 0.5 * recon
    return (error_out, factor, master_out)
```

```python
import functools

import jax
import jax.numpy as jnp
from jax import lax
from jax.experimental import pallas as pl
from jax.experimental.pallas import tpu as pltpu
from jax.sharding import PartitionSpec as P

ITERS = 3
LANES = 128
F32 = jnp.float32
BF16 = jnp.bfloat16
VMEM = pl.BlockSpec(memory_space=pltpu.VMEM)
ANY = pl.BlockSpec(memory_space=pltpu.HBM)
MIB = 1 << 20


def call(name, body, outs, *args, scratch=(), any_in=(), any_out=(), limit=8, flops=0):
    return pl.pallas_call(
        body,
        name=name,
        out_shape=[jax.ShapeDtypeStruct(s, d) for s, d in outs],
        in_specs=[ANY if i in any_in else VMEM for i in range(len(args))],
        out_specs=[ANY if i in any_out else VMEM for i in range(len(outs))],
        scratch_shapes=list(scratch),
        compiler_params=pltpu.CompilerParams(vmem_limit_bytes=limit * MIB),
        cost_estimate=pl.CostEstimate(flops=flops, bytes_accessed=0, transcendentals=0),
    )(*args)


def hop(x, mask, count):
    return lax.ppermute(x, "rep", [(i, i ^ mask) for i in range(count)])


def digit(shift, width):
    return lax.rem(lax.axis_index("rep") // (1 << shift), width)


def flip(value, mask, width):
    out = 0
    bit = 1
    while bit < width:
        b = lax.rem(value // bit, 2)
        out = out + bit * (1 - b if mask & bit else b)
        bit *= 2
    return out


def halves(x):
    high = x.astype(BF16)
    return high, (x - high.astype(F32)).astype(BF16)


def add_split(width, shift, a, b, *outs):
    d = digit(shift, width)
    h = outs[0].shape[0]
    for k, out in enumerate(outs):
        s = pl.ds(flip(d, k, width) * h, h)
        out[...] = a[s] + b[s]


def add_all(*refs):
    vals = [r[...] for r in refs[:-1]]
    while len(vals) > 1:
        vals = [vals[i] + vals[i + 1] for i in range(0, len(vals), 2)]
    refs[-1][...] = vals[0]


def gather(width, shift, *refs):
    d = digit(shift, width)
    out = refs[-1]
    h = refs[0].shape[0]
    for k, r in enumerate(refs[:-1]):
        out[pl.ds(flip(d, k, width) * h, h)] = r[...]


def finish_sum(keep, recv, count):
    m, rest = keep.shape[0], keep.shape[1:]
    width = min(4, count // 2)
    piece = ((m // width,) + rest, F32)
    parts = call("split", functools.partial(add_split, width, 1), [piece] * width, keep, recv)
    total = call("sum", add_all, [piece], parts[0], *[hop(parts[k], 2 * k, count) for k in range(1, width)])[0]
    shift = 1 + (width.bit_length() - 1)
    while (1 << shift) < count:
        w = min(4, count >> shift)
        total = call("sum", add_all, [piece], total, *[hop(total, k << shift, count) for k in range(1, w)])[0]
        shift += w.bit_length() - 1
    own = [total] + [hop(total, 2 * k, count) for k in range(1, width)]
    mine = call("gather", functools.partial(gather, width, 1), [((m,) + rest, F32)], *own)[0]
    return mine, hop(mine, 1, count)


def start_kernel(tile, x_hbm, dy_hbm, err_hbm, q_hbm, hi, lo, keep, send, x_v, xt_v, acc, pt, sem):
    depth = x_v.shape[0]
    rows, cols = hi.shape
    rank = q_hbm.shape[0]
    copy = pltpu.make_async_copy(x_hbm, x_v, sem)
    copy.start()
    acc[...] = jnp.zeros_like(acc)
    copy.wait()
    xt_v[...] = x_v[...].T
    step_rows = 256

    def body(idx, dy, err, q):
        (j,) = idx.index
        at = pl.ds(pl.multiple_of(j * tile, tile), tile)
        qh, ql = halves(q[...].T)
        right = jnp.concatenate([qh, ql], axis=1)
        for r in range(0, rows, step_rows):
            rs = pl.ds(r, step_rows)
            m = jnp.dot(xt_v[rs, :], dy[...], preferred_element_type=F32)
            m = m + err[rs, :].astype(F32)
            mh, ml = halves(m)
            hi[rs, at] = mh
            lo[rs, at] = ml
            acc[rs, :] += jnp.dot(mh, right, preferred_element_type=F32)
            acc[rs, 0:rank] += jnp.dot(ml, qh, preferred_element_type=F32)

    pltpu.emit_pipeline(
        body,
        grid=(cols // tile,),
        in_specs=[
            pl.BlockSpec((depth, tile), lambda j: (0, j)),
            pl.BlockSpec((rows, tile), lambda j: (0, j)),
            pl.BlockSpec((rank, tile), lambda j: (0, j)),
        ],
        _explicit_indices=True,
    )(dy_hbm, err_hbm, q_hbm)
    h = keep.shape[0]
    for b in range(rows // LANES):
        a = acc[b * LANES : (b + 1) * LANES, :]
        pt[b] = (a[:, 0:rank] + a[:, rank : 2 * rank]).T
    c = digit(0, 2)
    keep[...] = pt[pl.ds(c * h, h)]
    send[...] = pt[pl.ds((1 - c) * h, h)]


def right_kernel(scale, mine, other, out, tmp):
    c = digit(0, 2)
    h = mine.shape[0]
    rank = mine.shape[1]
    tmp[pl.ds(c * h, h)] = mine[...]
    tmp[pl.ds((1 - c) * h, h)] = other[...]
    for b in range(2 * h):
        qh, ql = halves((tmp[b] * scale).T)
        out[b * LANES : (b + 1) * LANES, 0:rank] = qh
        out[b * LANES : (b + 1) * LANES, rank : 2 * rank] = ql


def left_kernel(which, hi, lo, right, out):
    rank = right.shape[1] // 2
    h = out.shape[0]
    c = digit(0, 2)
    first = (c if which == 0 else 1 - c) * h * LANES
    for r in range(0, h * LANES, 256):
        rs = pl.ds(pl.multiple_of(first + r, 256), 256)
        a = jnp.dot(hi[rs, :], right[...], preferred_element_type=F32)
        b = jnp.dot(lo[rs, :], right[:, 0:rank], preferred_element_type=F32)
        p = a[:, 0:rank] + a[:, rank : 2 * rank] + b
        for i in range(256 // LANES):
            out[r // LANES + i] = p[i * LANES : (i + 1) * LANES].T


def basis_kernel(mine, other, out, tmp):
    c = digit(0, 2)
    h = mine.shape[0]
    rank = mine.shape[1]
    tmp[pl.ds(c * h, h)] = mine[...]
    tmp[pl.ds((1 - c) * h, h)] = other[...]
    blocks = 2 * h
    group = 8
    tiles = rank // group
    p = [[tmp[b, t * group : (t + 1) * group, :] for b in range(blocks)] for t in range(tiles)]
    v = [list(row) for row in p]
    row_of = lax.broadcasted_iota(jnp.int32, (group, 1), 0)
    for k in range(rank):
        t0, r0 = divmod(k, group)
        vk = [v[t0][b][r0 : r0 + 1, :] for b in range(blocks)]
        sq = functools.reduce(jnp.add, [x * x for x in vk])
        scale = lax.rsqrt(jnp.sum(sq, axis=1, keepdims=True) + 1.0)
        bk = [x * scale for x in vk]
        for t in range(t0, tiles):
            dots = functools.reduce(jnp.add, [p[t][b] * vk[b] for b in range(blocks)])
            coef = jnp.sum(dots, axis=1, keepdims=True) * scale
            if t == t0:
                coef = jnp.where(row_of > r0, coef, 0.0)
                here = row_of == r0
                v[t] = [jnp.where(here, bk[b], v[t][b] - coef * bk[b]) for b in range(blocks)]
            else:
                v[t] = [v[t][b] - coef * bk[b] for b in range(blocks)]
    for t in range(tiles):
        for b in range(blocks):
            out[t * group : (t + 1) * group, b * LANES : (b + 1) * LANES] = v[t][b]


def factor_kernel(which, tile, hi, lo, basis, out):
    rank = basis.shape[0]
    h = out.shape[0]
    c = digit(0, 2)
    first = (c if which == 0 else 1 - c) * h * LANES
    bh, bl = halves(basis[...])
    left = jnp.concatenate([bh, bl], axis=0)
    for j in range(0, h * LANES, tile):
        at = pl.ds(pl.multiple_of(first + j, tile), tile)
        a = jnp.dot(left, hi[:, at], preferred_element_type=F32)
        b = jnp.dot(bh, lo[:, at], preferred_element_type=F32)
        q = a[0:rank] + a[rank : 2 * rank] + b
        for i in range(tile // LANES):
            out[j // LANES + i] = q[:, i * LANES : (i + 1) * LANES]


def end_kernel(scale, tile, hi, lo, basis, mine, other, master, err_hbm, q_hbm, master_out, q_v, left_v, right_v, tmp):
    rows, cols = hi.shape
    rank = basis.shape[0]
    c = digit(0, 2)
    h = mine.shape[0]
    tmp[pl.ds(c * h, h)] = mine[...]
    tmp[pl.ds((1 - c) * h, h)] = other[...]
    bh, bl = halves(basis[...].T)
    left_v[...] = jnp.concatenate([bh, bl, bh], axis=1)
    for b in range(cols // LANES):
        q = tmp[b] * scale
        qh, ql = halves(q)
        q_v[:, b * LANES : (b + 1) * LANES] = q
        right_v[:, b * LANES : (b + 1) * LANES] = jnp.concatenate([qh, qh, ql], axis=0)
    width = master.shape[1]
    wide = max(width, LANES)
    begin = lax.axis_index("rep") * width
    own = pl.ds(pl.multiple_of(begin // wide * wide, wide), wide)
    recon = jnp.dot(left_v[...], right_v[:, own], preferred_element_type=F32)
    part = lax.rem(begin, wide) // width
    recon = functools.reduce(
        lambda kept, i: jnp.where(part == i, recon[:, i * width : (i + 1) * width], kept),
        range(1, wide // width),
        recon[:, 0:width],
    )
    master_out[...] = master[...] - 0.5 * recon

    def body(idx, err, q):
        (j,) = idx.index
        at = pl.ds(pl.multiple_of(j * tile, tile), tile)
        q[...] = q_v[:, at]
        for r in range(0, rows, 256):
            rs = pl.ds(r, 256)
            rec = jnp.dot(left_v[rs, :], right_v[:, at], preferred_element_type=F32)
            m = hi[rs, at].astype(F32) + lo[rs, at].astype(F32)
            err[rs, :] = (m - rec).astype(BF16)

    pltpu.emit_pipeline(
        body,
        grid=(cols // tile,),
        in_specs=[],
        out_specs=[
            pl.BlockSpec((rows, tile), lambda j: (0, j)),
            pl.BlockSpec((rank, tile), lambda j: (0, j)),
        ],
        _explicit_indices=True,
    )(err_hbm, q_hbm)


def shards(inputs, out_grads, error_in, q_start, master):
    count = lax.axis_size("rep")
    depth, rows = inputs.shape
    cols = out_grads.shape[1]
    rank = q_start.shape[0]
    p_blocks, q_blocks = rows // LANES, cols // LANES
    p_half = ((p_blocks // 2, rank, LANES), F32)
    q_half = ((q_blocks // 2, rank, LANES), F32)
    work = 3 * rows * cols * rank
    tile = 512
    hi, lo, keep, send = call(
        "start",
        functools.partial(start_kernel, tile),
        [((rows, cols), BF16), ((rows, cols), BF16), p_half, p_half],
        inputs,
        out_grads,
        error_in.reshape(rows, cols),
        q_start,
        any_in=(0, 1, 2, 3),
        scratch=[
            pltpu.VMEM((depth, rows), BF16),
            pltpu.VMEM((rows, depth), BF16),
            pltpu.VMEM((rows, 2 * rank), F32),
            pltpu.VMEM((p_blocks, rank, LANES), F32),
            pltpu.SemaphoreType.DMA,
        ],
        limit=46,
        flops=2 * depth * rows * cols,
    )
    recv = hop(send, 1, count)
    for step in range(ITERS):
        mine, other = finish_sum(keep, recv, count)
        basis = call("basis", basis_kernel, [((rank, rows), F32)], mine, other,
                     scratch=[pltpu.VMEM((p_blocks, rank, LANES), F32)], flops=work)[0]
        send = call("factor", functools.partial(factor_kernel, 1, tile), [q_half], hi, lo, basis, flops=work)[0]
        recv = hop(send, 1, count)
        keep = call("factor", functools.partial(factor_kernel, 0, tile), [q_half], hi, lo, basis, flops=work)[0]
        mine, other = finish_sum(keep, recv, count)
        if step + 1 < ITERS:
            right = call("right", functools.partial(right_kernel, 1.0 / count), [((cols, 2 * rank), BF16)], mine, other,
                         scratch=[pltpu.VMEM((q_blocks, rank, LANES), F32)])[0]
            send = call("left", functools.partial(left_kernel, 1), [p_half], hi, lo, right, flops=work)[0]
            recv = hop(send, 1, count)
            keep = call("left", functools.partial(left_kernel, 0), [p_half], hi, lo, right, flops=work)[0]
    error_out, q_out, master_out = call(
        "end",
        functools.partial(end_kernel, 1.0 / count, tile),
        [((rows, cols), BF16), ((rank, cols), F32), (master.shape, F32)],
        hi, lo, basis, mine, other, master,
        any_out=(0, 1),
        scratch=[
            pltpu.VMEM((rank, cols), F32),
            pltpu.VMEM((rows, 3 * rank), BF16),
            pltpu.VMEM((3 * rank, cols), BF16),
            pltpu.VMEM((q_blocks, rank, LANES), F32),
        ],
        limit=16,
        flops=work,
    )
    return error_out[None], q_out, master_out


def solution(mesh):
    def step(*args):
        with jax.sharding.use_abstract_mesh(mesh.abstract_mesh):
            return jax.shard_map(
                shards,
                mesh=mesh,
                in_specs=(P("rep", None), P("rep", None), P("rep", None, None), P(), P(None, "rep")),
                out_specs=(P("rep", None, None), P(), P(None, "rep")),
                check_vma=False,
            )(*args)

    return step
```

```python
import functools

import jax
import jax.numpy as jnp
from jax import lax
from jax.experimental import pallas as pl
from jax.experimental.pallas import tpu as pltpu
from jax.sharding import PartitionSpec as P

ITERS = 3
LANES = 128
F32 = jnp.float32
BF16 = jnp.bfloat16
VMEM = pl.BlockSpec(memory_space=pltpu.VMEM)
ANY = pl.BlockSpec(memory_space=pltpu.HBM)
MIB = 1 << 20


def call(name, body, outs, *args, scratch=(), any_in=(), any_out=(), limit=8, flops=0):
    return pl.pallas_call(
        body,
        name=name,
        out_shape=[(pltpu.HBM if i in any_out else pltpu.VMEM)(s, d) for i, (s, d) in enumerate(outs)],
        in_specs=[ANY if i in any_in else VMEM for i in range(len(args))],
        out_specs=[ANY if i in any_out else VMEM for i in range(len(outs))],
        scratch_shapes=list(scratch),
        compiler_params=pltpu.CompilerParams(vmem_limit_bytes=limit * MIB),
        cost_estimate=pl.CostEstimate(flops=flops, bytes_accessed=0, transcendentals=0),
    )(*[pltpu.with_memory_space_constraint(a, pltpu.HBM) if i in any_in else a for i, a in enumerate(args)])


def hop(x, mask, count):
    return lax.ppermute(x, "rep", [(i, i ^ mask) for i in range(count)])


def digit(shift, width):
    return lax.rem(lax.axis_index("rep") // (1 << shift), width)


def flip(value, mask, width):
    out = 0
    bit = 1
    while bit < width:
        b = lax.rem(value // bit, 2)
        out = out + bit * (1 - b if mask & bit else b)
        bit *= 2
    return out


def halves(x):
    high = x.astype(BF16)
    return high, (x - high.astype(F32)).astype(BF16)


def add_split(width, shift, a, b, *outs):
    d = digit(shift, width)
    h = outs[0].shape[0]
    for k, out in enumerate(outs):
        s = pl.ds(flip(d, k, width) * h, h)
        out[...] = a[s] + b[s]


def add_all(*refs):
    vals = [r[...] for r in refs[:-1]]
    while len(vals) > 1:
        vals = [vals[i] + vals[i + 1] for i in range(0, len(vals), 2)]
    refs[-1][...] = vals[0]


def gather(width, shift, *refs):
    d = digit(shift, width)
    out = refs[-1]
    h = refs[0].shape[0]
    for k, r in enumerate(refs[:-1]):
        out[pl.ds(flip(d, k, width) * h, h)] = r[...]


def finish_sum(keep, recv, count):
    m, rest = keep.shape[0], keep.shape[1:]
    width = min(4, count // 2)
    piece = ((m // width,) + rest, F32)
    parts = call("split", functools.partial(add_split, width, 1), [piece] * width, keep, recv)
    total = call("sum", add_all, [piece], parts[0], *[hop(parts[k], 2 * k, count) for k in range(1, width)])[0]
    shift = 1 + (width.bit_length() - 1)
    while (1 << shift) < count:
        w = min(4, count >> shift)
        total = call("sum", add_all, [piece], total, *[hop(total, k << shift, count) for k in range(1, w)])[0]
        shift += w.bit_length() - 1
    own = [total] + [hop(total, 2 * k, count) for k in range(1, width)]
    mine = call("gather", functools.partial(gather, width, 1), [((m,) + rest, F32)], *own)[0]
    return mine, hop(mine, 1, count)


def start_kernel(tile, step_rows, x_hbm, dy_hbm, err_hbm, q_hbm, hi, lo, keep, send, x_v, xt_v, acc, pt, sem):
    depth = x_v.shape[0]
    rows, cols = hi.shape
    rank = q_hbm.shape[0]
    copy = pltpu.make_async_copy(x_hbm, x_v, sem)
    copy.start()
    acc[...] = jnp.zeros_like(acc)

    def body(idx, dy, err, q):
        (j,) = idx.index

        @pl.when(j == 0)
        def _():
            copy.wait()
            xt_v[...] = x_v[...].T

        at = pl.ds(pl.multiple_of(j * tile, tile), tile)
        qh, ql = halves(q[...].T)
        right = jnp.concatenate([qh, ql], axis=1)
        for r in range(0, rows, step_rows):
            rs = pl.ds(r, step_rows)
            m = jnp.dot(xt_v[rs, :], dy[...], preferred_element_type=F32)
            m = m + err[rs, :].astype(F32)
            mh, ml = halves(m)
            hi[rs, at] = mh
            lo[rs, at] = ml
            acc[rs, :] += jnp.dot(mh, right, preferred_element_type=F32)
            acc[rs, 0:rank] += jnp.dot(ml, qh, preferred_element_type=F32)

    pltpu.emit_pipeline(
        body,
        grid=(cols // tile,),
        in_specs=[
            pl.BlockSpec((depth, tile), lambda j: (0, j)),
            pl.BlockSpec((rows, tile), lambda j: (0, j)),
            pl.BlockSpec((rank, tile), lambda j: (0, j)),
        ],
        _explicit_indices=True,
    )(dy_hbm, err_hbm, q_hbm)
    h = keep.shape[0]
    for b in range(rows // LANES):
        a = acc[b * LANES : (b + 1) * LANES, :]
        pt[b] = (a[:, 0:rank] + a[:, rank : 2 * rank]).T
    c = digit(0, 2)
    keep[...] = pt[pl.ds(c * h, h)]
    send[...] = pt[pl.ds((1 - c) * h, h)]


def right_kernel(scale, mine, other, out, tmp):
    c = digit(0, 2)
    h = mine.shape[0]
    rank = mine.shape[1]
    tmp[pl.ds(c * h, h)] = mine[...]
    tmp[pl.ds((1 - c) * h, h)] = other[...]
    for b in range(2 * h):
        qh, ql = halves((tmp[b] * scale).T)
        out[b * LANES : (b + 1) * LANES, 0:rank] = qh
        out[b * LANES : (b + 1) * LANES, rank : 2 * rank] = ql


def left_kernel(which, hi, lo, right, out):
    rank = right.shape[1] // 2
    h = out.shape[0]
    c = digit(0, 2)
    first = (c if which == 0 else 1 - c) * h * LANES
    for r in range(0, h * LANES, 256):
        rs = pl.ds(pl.multiple_of(first + r, 256), 256)
        a = jnp.dot(hi[rs, :], right[...], preferred_element_type=F32)
        b = jnp.dot(lo[rs, :], right[:, 0:rank], preferred_element_type=F32)
        p = a[:, 0:rank] + a[:, rank : 2 * rank] + b
        for i in range(256 // LANES):
            out[r // LANES + i] = p[i * LANES : (i + 1) * LANES].T


def basis_kernel(mine, other, out, tmp):
    c = digit(0, 2)
    h = mine.shape[0]
    rank = mine.shape[1]
    tmp[pl.ds(c * h, h)] = mine[...]
    tmp[pl.ds((1 - c) * h, h)] = other[...]
    blocks = 2 * h
    group = 8
    tiles = rank // group
    p = [[tmp[b, t * group : (t + 1) * group, :] for b in range(blocks)] for t in range(tiles)]
    v = [list(row) for row in p]
    row_of = lax.broadcasted_iota(jnp.int32, (group, 1), 0)
    for k in range(rank):
        t0, r0 = divmod(k, group)
        vk = [v[t0][b][r0 : r0 + 1, :] for b in range(blocks)]
        sq = functools.reduce(jnp.add, [x * x for x in vk])
        scale = lax.rsqrt(jnp.sum(sq, axis=1, keepdims=True) + 1.0)
        bk = [x * scale for x in vk]
        for t in range(t0, tiles):
            dots = functools.reduce(jnp.add, [p[t][b] * vk[b] for b in range(blocks)])
            coef = jnp.sum(dots, axis=1, keepdims=True) * scale
            if t == t0:
                coef = jnp.where(row_of > r0, coef, 0.0)
                here = row_of == r0
                v[t] = [jnp.where(here, bk[b], v[t][b] - coef * bk[b]) for b in range(blocks)]
            else:
                v[t] = [v[t][b] - coef * bk[b] for b in range(blocks)]
    for t in range(tiles):
        for b in range(blocks):
            out[t * group : (t + 1) * group, b * LANES : (b + 1) * LANES] = v[t][b]


def factor_kernel(which, tile, hi, lo, basis, out):
    rank = basis.shape[0]
    h = out.shape[0]
    c = digit(0, 2)
    first = (c if which == 0 else 1 - c) * h * LANES
    bh, bl = halves(basis[...])
    left = jnp.concatenate([bh, bl], axis=0)
    for j in range(0, h * LANES, tile):
        at = pl.ds(pl.multiple_of(first + j, tile), tile)
        a = jnp.dot(left, hi[:, at], preferred_element_type=F32)
        b = jnp.dot(bh, lo[:, at], preferred_element_type=F32)
        q = a[0:rank] + a[rank : 2 * rank] + b
        for i in range(tile // LANES):
            out[j // LANES + i] = q[:, i * LANES : (i + 1) * LANES]


def end_kernel(scale, tile, hi, lo, basis, mine, other, master, err_hbm, q_hbm, master_out, q_v, left_v, right_v, tmp, master_v, sem):
    rows, cols = hi.shape
    rank = basis.shape[0]
    c = digit(0, 2)
    h = mine.shape[0]
    tmp[pl.ds(c * h, h)] = mine[...]
    tmp[pl.ds((1 - c) * h, h)] = other[...]
    bh, bl = halves(basis[...].T)
    left_v[...] = jnp.concatenate([bh, bl, bh], axis=1)
    for b in range(cols // LANES):
        q = tmp[b] * scale
        qh, ql = halves(q)
        q_v[:, b * LANES : (b + 1) * LANES] = q
        right_v[:, b * LANES : (b + 1) * LANES] = jnp.concatenate([qh, qh, ql], axis=0)
    width = master.shape[1]
    wide = max(width, LANES)
    begin = lax.axis_index("rep") * width
    own = pl.ds(pl.multiple_of(begin // wide * wide, wide), wide)
    recon = jnp.dot(left_v[...], right_v[:, own], preferred_element_type=F32)
    part = lax.rem(begin, wide) // width
    recon = functools.reduce(
        lambda kept, i: jnp.where(part == i, recon[:, i * width : (i + 1) * width], kept),
        range(1, wide // width),
        recon[:, 0:width],
    )
    master_v[...] = master[...] - 0.5 * recon
    copy = pltpu.make_async_copy(master_v, master_out, sem)
    copy.start()

    def body(idx, err, q):
        (j,) = idx.index
        at = pl.ds(pl.multiple_of(j * tile, tile), tile)
        q[...] = q_v[:, at]
        for r in range(0, rows, 256):
            rs = pl.ds(r, 256)
            rec = jnp.dot(left_v[rs, :], right_v[:, at], preferred_element_type=F32)
            m = hi[rs, at].astype(F32) + lo[rs, at].astype(F32)
            err[rs, :] = (m - rec).astype(BF16)

    pltpu.emit_pipeline(
        body,
        grid=(cols // tile,),
        in_specs=[],
        out_specs=[
            pl.BlockSpec((rows, tile), lambda j: (0, j)),
            pl.BlockSpec((rank, tile), lambda j: (0, j)),
        ],
        _explicit_indices=True,
    )(err_hbm, q_hbm)
    copy.wait()


def shards(inputs, out_grads, error_in, q_start, master):
    count = lax.axis_size("rep")
    depth, rows = inputs.shape
    cols = out_grads.shape[1]
    rank = q_start.shape[0]
    p_blocks, q_blocks = rows // LANES, cols // LANES
    p_half = ((p_blocks // 2, rank, LANES), F32)
    q_half = ((q_blocks // 2, rank, LANES), F32)
    work = 3 * rows * cols * rank
    tile = 512
    hi, lo, keep, send = call(
        "start",
        functools.partial(start_kernel, tile, 1024),
        [((rows, cols), BF16), ((rows, cols), BF16), p_half, p_half],
        inputs,
        out_grads,
        error_in.reshape(rows, cols),
        q_start,
        any_in=(0, 1, 2, 3),
        scratch=[
            pltpu.VMEM((depth, rows), BF16),
            pltpu.VMEM((rows, depth), BF16),
            pltpu.VMEM((rows, 2 * rank), F32),
            pltpu.VMEM((p_blocks, rank, LANES), F32),
            pltpu.SemaphoreType.DMA,
        ],
        limit=24,
        flops=2 * depth * rows * cols,
    )
    recv = hop(send, 1, count)
    for step in range(ITERS):
        mine, other = finish_sum(keep, recv, count)
        basis = call("basis", basis_kernel, [((rank, rows), F32)], mine, other,
                     scratch=[pltpu.VMEM((p_blocks, rank, LANES), F32)], flops=work)[0]
        send = call("factor", functools.partial(factor_kernel, 1, tile), [q_half], hi, lo, basis, flops=work)[0]
        recv = hop(send, 1, count)
        keep = call("factor", functools.partial(factor_kernel, 0, tile), [q_half], hi, lo, basis, flops=work)[0]
        mine, other = finish_sum(keep, recv, count)
        if step + 1 < ITERS:
            right = call("right", functools.partial(right_kernel, 1.0 / count), [((cols, 2 * rank), BF16)], mine, other,
                         scratch=[pltpu.VMEM((q_blocks, rank, LANES), F32)])[0]
            send = call("left", functools.partial(left_kernel, 1), [p_half], hi, lo, right, flops=work)[0]
            recv = hop(send, 1, count)
            keep = call("left", functools.partial(left_kernel, 0), [p_half], hi, lo, right, flops=work)[0]
    error_out, q_out, master_out = call(
        "end",
        functools.partial(end_kernel, 1.0 / count, tile),
        [((rows, cols), BF16), ((rank, cols), F32), (master.shape, F32)],
        hi, lo, basis, mine, other, master,
        any_out=(0, 1, 2),
        scratch=[
            pltpu.VMEM((rank, cols), F32),
            pltpu.VMEM((rows, 3 * rank), BF16),
            pltpu.VMEM((3 * rank, cols), BF16),
            pltpu.VMEM((q_blocks, rank, LANES), F32),
            pltpu.VMEM(master.shape, F32),
            pltpu.SemaphoreType.DMA,
        ],
        limit=16,
        flops=work,
    )
    return error_out[None], q_out, master_out


def solution(mesh):
    def step(*args):
        with jax.sharding.use_abstract_mesh(mesh.abstract_mesh):
            return jax.shard_map(
                shards,
                mesh=mesh,
                in_specs=(P("rep", None), P("rep", None), P("rep", None, None), P(), P(None, "rep")),
                out_specs=(P("rep", None, None), P(), P(None, "rep")),
                check_vma=False,
            )(*args)

    return step
```

```python
import functools

import jax
import jax.numpy as jnp
from jax import lax
from jax.experimental import pallas as pl
from jax.experimental.pallas import tpu as pltpu
from jax.sharding import PartitionSpec as P

ITERS = 3
LANES = 128
F32 = jnp.float32
BF16 = jnp.bfloat16
VMEM = pl.BlockSpec(memory_space=pltpu.VMEM)
ANY = pl.BlockSpec(memory_space=pltpu.HBM)
MIB = 1 << 20


def call(name, body, outs, *args, scratch=(), any_in=(), any_out=(), limit=8, flops=0):
    return pl.pallas_call(
        body,
        name=name,
        out_shape=[(pltpu.HBM if i in any_out else pltpu.VMEM)(s, d) for i, (s, d) in enumerate(outs)],
        in_specs=[ANY if i in any_in else VMEM for i in range(len(args))],
        out_specs=[ANY if i in any_out else VMEM for i in range(len(outs))],
        scratch_shapes=list(scratch),
        compiler_params=pltpu.CompilerParams(vmem_limit_bytes=limit * MIB),
        cost_estimate=pl.CostEstimate(flops=flops, bytes_accessed=0, transcendentals=0),
    )(*[pltpu.with_memory_space_constraint(a, pltpu.HBM) if i in any_in else a for i, a in enumerate(args)])


def hop(x, mask, count):
    return lax.ppermute(x, "rep", [(i, i ^ mask) for i in range(count)])


def digit(shift, width):
    return lax.rem(lax.axis_index("rep") // (1 << shift), width)


def flip(value, mask, width):
    out = 0
    bit = 1
    while bit < width:
        b = lax.rem(value // bit, 2)
        out = out + bit * (1 - b if mask & bit else b)
        bit *= 2
    return out


def odd_bits(count):
    return [b for b in range(1, count.bit_length() - 1) if b < 4 or b % 2]


def part_of(count):
    me = lax.axis_index("rep")
    return lax.rem(sum((lax.rem(me // (1 << b), 2) for b in odd_bits(count)), lax.rem(me, 2)), 2)


def chip_hop(x, mask, count):
    turn = sum((mask >> b) & 1 for b in odd_bits(count)) % 2
    return hop(x, mask | turn, count)


def halves(x):
    high = x.astype(BF16)
    return high, (x - high.astype(F32)).astype(BF16)


def add_split(width, shift, a, b, *outs):
    d = digit(shift, width)
    h = outs[0].shape[0]
    for k, out in enumerate(outs):
        s = pl.ds(flip(d, k, width) * h, h)
        out[...] = a[s] + b[s]


def add_all(*refs):
    vals = [r[...] for r in refs[:-1]]
    while len(vals) > 1:
        vals = [vals[i] + vals[i + 1] for i in range(0, len(vals), 2)]
    refs[-1][...] = vals[0]


def gather(width, shift, *refs):
    d = digit(shift, width)
    out = refs[-1]
    h = refs[0].shape[0]
    for k, r in enumerate(refs[:-1]):
        out[pl.ds(flip(d, k, width) * h, h)] = r[...]


def sum_parts(parts, rest_shift, count):
    width = len(parts)
    piece = (parts[0].shape, F32)
    total = call("sum", add_all, [piece], parts[0], *[chip_hop(parts[k], 2 * k, count) for k in range(1, width)])[0]
    shift = rest_shift
    while (1 << shift) < count:
        w = min(4, count >> shift)
        total = call("sum", add_all, [piece], total, *[chip_hop(total, k << shift, count) for k in range(1, w)])[0]
        shift += w.bit_length() - 1
    own = [total] + [chip_hop(total, 2 * k, count) for k in range(1, width)]
    half = ((width * piece[0][0],) + piece[0][1:], F32)
    return call("gather", functools.partial(gather, width, 1), [half], *own)[0]


def sum_pair(keep, recv, width, rest_shift, count):
    piece = ((keep.shape[0] // width,) + keep.shape[1:], F32)
    parts = call("split", functools.partial(add_split, width, 1), [piece] * width, keep, recv)
    return sum_parts(parts, rest_shift, count)


def start_kernel(tile, step_rows, count, x_hbm, dy_hbm, err_hbm, q_hbm, own, give, keep, send, x_v, xt_v, acc, pt, sem):
    depth = x_v.shape[0]
    rows = own.shape[0]
    cols = dy_hbm.shape[1]
    rank = q_hbm.shape[0]
    c = part_of(count)
    steps = own.shape[1] // tile
    copy = pltpu.make_async_copy(x_hbm, x_v, sem)
    copy.start()
    acc[...] = jnp.zeros_like(acc)

    def body(idx, dy, err, q):
        (j,) = idx.index

        @pl.when(j == 0)
        def _():
            copy.wait()
            xt_v[...] = x_v[...].T

        def part(to):
            at = pl.ds(pl.multiple_of(lax.rem(j, steps) * tile, tile), tile)
            qh, ql = halves(q[...].T)
            right = jnp.concatenate([qh, ql], axis=1)
            for r in range(0, rows, step_rows):
                rs = pl.ds(r, step_rows)
                m = jnp.dot(xt_v[rs, :], dy[...], preferred_element_type=F32)
                m = m + err[rs, :].astype(F32)
                to[rs, at] = m
                mh, ml = halves(m)
                acc[rs, :] += jnp.dot(mh, right, preferred_element_type=F32)
                acc[rs, 0:rank] += jnp.dot(ml, qh, preferred_element_type=F32)

        pl.when(j // steps == c)(functools.partial(part, own))
        pl.when(j // steps != c)(functools.partial(part, give))

    pltpu.emit_pipeline(
        body,
        grid=(cols // tile,),
        in_specs=[
            pl.BlockSpec((depth, tile), lambda j: (0, j)),
            pl.BlockSpec((rows, tile), lambda j: (0, j)),
            pl.BlockSpec((rank, tile), lambda j: (0, j)),
        ],
        _explicit_indices=True,
    )(dy_hbm, err_hbm, q_hbm)
    h = keep.shape[0]
    for b in range(rows // LANES):
        a = acc[b * LANES : (b + 1) * LANES, :]
        pt[b] = (a[:, 0:rank] + a[:, rank : 2 * rank]).T
    keep[...] = pt[pl.ds(c * h, h)]
    send[...] = pt[pl.ds((1 - c) * h, h)]


def pair_kernel(tile, own, got, hi, lo):
    def body(j, carry):
        at = pl.ds(pl.multiple_of(j * tile, tile), tile)
        hi[:, at], lo[:, at] = halves(own[:, at] + got[:, at])
        return carry

    lax.fori_loop(0, own.shape[1] // tile, body, 0)


def right_kernel(scale, mine, out):
    rank = mine.shape[1]
    for b in range(mine.shape[0]):
        qh, ql = halves((mine[b] * scale).T)
        out[b * LANES : (b + 1) * LANES, 0:rank] = qh
        out[b * LANES : (b + 1) * LANES, rank : 2 * rank] = ql


def left_kernel(which, count, hi, lo, right, out):
    rank = right.shape[1] // 2
    h = out.shape[0]
    c = part_of(count)
    first = (c if which == 0 else 1 - c) * h * LANES
    for r in range(0, h * LANES, 256):
        rs = pl.ds(pl.multiple_of(first + r, 256), 256)
        a = jnp.dot(hi[rs, :], right[...], preferred_element_type=F32)
        b = jnp.dot(lo[rs, :], right[:, 0:rank], preferred_element_type=F32)
        p = a[:, 0:rank] + a[:, rank : 2 * rank] + b
        for i in range(256 // LANES):
            out[r // LANES + i] = p[i * LANES : (i + 1) * LANES].T


def basis_kernel(count, mine, other, out, tmp):
    c = part_of(count)
    h = mine.shape[0]
    rank = mine.shape[1]
    tmp[pl.ds(c * h, h)] = mine[...]
    tmp[pl.ds((1 - c) * h, h)] = other[...]
    blocks = 2 * h
    group = 8
    tiles = rank // group
    p = [[tmp[b, t * group : (t + 1) * group, :] for b in range(blocks)] for t in range(tiles)]
    v = [list(row) for row in p]
    row_of = lax.broadcasted_iota(jnp.int32, (group, 1), 0)
    for k in range(rank):
        t0, r0 = divmod(k, group)
        vk = [v[t0][b][r0 : r0 + 1, :] for b in range(blocks)]
        sq = functools.reduce(jnp.add, [x * x for x in vk])
        scale = lax.rsqrt(jnp.sum(sq, axis=1, keepdims=True) + 1.0)
        bk = [x * scale for x in vk]
        for t in range(t0, tiles):
            dots = functools.reduce(jnp.add, [p[t][b] * vk[b] for b in range(blocks)])
            coef = jnp.sum(dots, axis=1, keepdims=True) * scale
            if t == t0:
                coef = jnp.where(row_of > r0, coef, 0.0)
                here = row_of == r0
                v[t] = [jnp.where(here, bk[b], v[t][b] - coef * bk[b]) for b in range(blocks)]
            else:
                v[t] = [v[t][b] - coef * bk[b] for b in range(blocks)]
    for t in range(tiles):
        for b in range(blocks):
            out[t * group : (t + 1) * group, b * LANES : (b + 1) * LANES] = v[t][b]


def factor_kernel(picks, width, hi, lo, basis, *outs):
    rank = basis.shape[0]
    h = outs[0].shape[0]
    d = digit(1, width)
    bh, bl = halves(basis[...])
    left = jnp.concatenate([bh, bl], axis=0)
    for k, out in zip(picks, outs):
        at = pl.ds(pl.multiple_of(flip(d, k, width) * (h * LANES), h * LANES), h * LANES)
        a = jnp.dot(left, hi[:, at], preferred_element_type=F32)
        b = jnp.dot(bh, lo[:, at], preferred_element_type=F32)
        q = a[0:rank] + a[rank : 2 * rank] + b
        for i in range(h):
            out[i] = q[:, i * LANES : (i + 1) * LANES]


def end_kernel(scale, tile, count, own, give, basis, mine, other, master, err_hbm, q_hbm, master_out, q_v, left_v, right_v, tmp, master_v, sem):
    rows, cols = own.shape[0], 2 * own.shape[1]
    steps = own.shape[1] // tile
    rank = basis.shape[0]
    c = part_of(count)
    h = mine.shape[0]
    tmp[pl.ds(c * h, h)] = mine[...]
    tmp[pl.ds((1 - c) * h, h)] = other[...]
    bh, bl = halves(basis[...].T)
    left_v[...] = jnp.concatenate([bh, bl, bh], axis=1)
    for b in range(cols // LANES):
        q = tmp[b] * scale
        qh, ql = halves(q)
        q_v[:, b * LANES : (b + 1) * LANES] = q
        right_v[:, b * LANES : (b + 1) * LANES] = jnp.concatenate([qh, qh, ql], axis=0)
    width = master.shape[1]
    wide = max(width, LANES)
    begin = lax.axis_index("rep") * width
    at = pl.ds(pl.multiple_of(begin // wide * wide, wide), wide)
    recon = jnp.dot(left_v[...], right_v[:, at], preferred_element_type=F32)
    part = lax.rem(begin, wide) // width
    recon = functools.reduce(
        lambda kept, i: jnp.where(part == i, recon[:, i * width : (i + 1) * width], kept),
        range(1, wide // width),
        recon[:, 0:width],
    )
    master_v[...] = master[...] - 0.5 * recon
    copy = pltpu.make_async_copy(master_v, master_out, sem)
    copy.start()

    def body(idx, err, q):
        (j,) = idx.index
        at = pl.ds(pl.multiple_of(j * tile, tile), tile)
        q[...] = q_v[:, at]

        def part(merged):
            here = pl.ds(pl.multiple_of(lax.rem(j, steps) * tile, tile), tile)
            for r in range(0, rows, 256):
                rs = pl.ds(r, 256)
                rec = jnp.dot(left_v[rs, :], right_v[:, at], preferred_element_type=F32)
                err[rs, :] = (merged[rs, here] - rec).astype(BF16)

        pl.when(j // steps == c)(functools.partial(part, own))
        pl.when(j // steps != c)(functools.partial(part, give))

    pltpu.emit_pipeline(
        body,
        grid=(cols // tile,),
        in_specs=[],
        out_specs=[
            pl.BlockSpec((rows, tile), lambda j: (0, j)),
            pl.BlockSpec((rank, tile), lambda j: (0, j)),
        ],
        _explicit_indices=True,
    )(err_hbm, q_hbm)
    copy.wait()


def shards(inputs, out_grads, error_in, q_start, master):
    count = lax.axis_size("rep")
    depth, rows = inputs.shape
    cols = out_grads.shape[1]
    rank = q_start.shape[0]
    p_blocks, q_blocks = rows // LANES, cols // LANES
    p_half = ((p_blocks // 2, rank, LANES), F32)
    width = min(4, count // 2)
    rest = width.bit_length()
    q_piece = ((q_blocks // 2 // width, rank, LANES), F32)
    half = (rows, cols // 2)
    work = 3 * rows * cols * rank
    tile = 512
    own, give, keep, send = call(
        "start",
        functools.partial(start_kernel, tile, 1024, count),
        [(half, F32), (half, F32), p_half, p_half],
        inputs,
        out_grads,
        error_in.reshape(rows, cols),
        q_start,
        any_in=(0, 1, 2, 3),
        scratch=[
            pltpu.VMEM((depth, rows), BF16),
            pltpu.VMEM((rows, depth), BF16),
            pltpu.VMEM((rows, 2 * rank), F32),
            pltpu.VMEM((p_blocks, rank, LANES), F32),
            pltpu.SemaphoreType.DMA,
        ],
        limit=16,
        flops=2 * depth * rows * cols,
    )
    recv, give = lax.optimization_barrier((hop(send, 1, count), give))
    got = hop(give, 1, count)
    for step in range(ITERS):
        mine = sum_pair(keep, recv, width, rest, count)
        other = hop(mine, 1, count)
        basis = call("basis", functools.partial(basis_kernel, count), [((rank, rows), F32)], mine, other,
                     scratch=[pltpu.VMEM((p_blocks, rank, LANES), F32)], flops=work)[0]
        if step == 0:
            pair = call("pair", functools.partial(pair_kernel, tile // 2), [(half, BF16), (half, BF16)], own, got, flops=work)
        picks = list(range(1, width))
        away = call("factor", functools.partial(factor_kernel, picks, width), [q_piece] * len(picks), *pair, basis, flops=work)
        home = call("factor", functools.partial(factor_kernel, [0], width), [q_piece], *pair, basis, flops=work)
        mine = sum_parts([*home, *away], rest, count)
        if step + 1 < ITERS:
            right = call("right", functools.partial(right_kernel, 1.0 / count), [((half[1], 2 * rank), BF16)], mine)[0]
            send = call("left", functools.partial(left_kernel, 1, count), [p_half], *pair, right, flops=work)[0]
            recv = hop(send, 1, count)
            keep = call("left", functools.partial(left_kernel, 0, count), [p_half], *pair, right, flops=work)[0]
    other = hop(mine, 1, count)
    error_out, q_out, master_out = call(
        "end",
        functools.partial(end_kernel, 1.0 / count, tile, count),
        [((rows, cols), BF16), ((rank, cols), F32), (master.shape, F32)],
        own, give, basis, mine, other, master,
        any_out=(0, 1, 2),
        scratch=[
            pltpu.VMEM((rank, cols), F32),
            pltpu.VMEM((rows, 3 * rank), BF16),
            pltpu.VMEM((3 * rank, cols), BF16),
            pltpu.VMEM((q_blocks, rank, LANES), F32),
            pltpu.VMEM(master.shape, F32),
            pltpu.SemaphoreType.DMA,
        ],
        limit=16,
        flops=work,
    )
    return error_out[None], q_out, master_out


def solution(mesh):
    def step(*args):
        with jax.sharding.use_abstract_mesh(mesh.abstract_mesh):
            return jax.shard_map(
                shards,
                mesh=mesh,
                in_specs=(P("rep", None), P("rep", None), P("rep", None, None), P(), P(None, "rep")),
                out_specs=(P("rep", None, None), P(), P(None, "rep")),
                check_vma=False,
            )(*args)

    return step
```

```python
import functools

import jax
import jax.numpy as jnp
from jax import lax
from jax.experimental import pallas as pl
from jax.experimental.pallas import tpu as pltpu
from jax.sharding import PartitionSpec as P


ITERS = 3
LANES = 128
F32 = jnp.float32
BF16 = jnp.bfloat16
VMEM = pl.BlockSpec(memory_space=pltpu.VMEM)
ANY = pl.BlockSpec(memory_space=pltpu.HBM)
MIB = 1 << 20


def call(body, outs, *args, scratch=(), any_in=(), any_out=(), limit=8, flops=0):
    return pl.pallas_call(
        body,
        out_shape=[(pltpu.HBM if i in any_out else pltpu.VMEM)(s, d) for i, (s, d) in enumerate(outs)],
        in_specs=[ANY if i in any_in else VMEM for i in range(len(args))],
        out_specs=[ANY if i in any_out else VMEM for i in range(len(outs))],
        scratch_shapes=list(scratch),
        compiler_params=pltpu.CompilerParams(vmem_limit_bytes=limit * MIB),
        cost_estimate=pl.CostEstimate(flops=flops, bytes_accessed=0, transcendentals=0),
    )(*[pltpu.with_memory_space_constraint(a, pltpu.HBM) if i in any_in else a for i, a in enumerate(args)])


def hop(x, mask, count):
    return lax.ppermute(x, "rep", [(i, i ^ mask) for i in range(count)])


def digit(shift, width):
    return lax.rem(lax.axis_index("rep") // (1 << shift), width)


def flip(value, mask, width):
    out = 0
    bit = 1
    while bit < width:
        b = lax.rem(value // bit, 2)
        out = out + bit * (1 - b if mask & bit else b)
        bit *= 2
    return out


def thirds(x):
    high = x.astype(BF16)
    rest = x - high.astype(F32)
    mid = rest.astype(BF16)
    return [high, mid, (rest - mid.astype(F32)).astype(BF16)]


def joined(count, mine, other):
    c = part_of(count)
    h = mine.shape[0]
    first = [jnp.where(c == 0, mine[b], other[b]) for b in range(h)]
    second = [jnp.where(c == 0, other[b], mine[b]) for b in range(h)]
    return jnp.concatenate(first + second, axis=1)


def odd_bits(count):
    return [b for b in range(1, count.bit_length() - 1) if b < 4 or b % 2]


def part_of(count):
    me = lax.axis_index("rep")
    return lax.rem(sum((lax.rem(me // (1 << b), 2) for b in odd_bits(count)), lax.rem(me, 2)), 2)


def chip_hop(x, mask, count):
    turn = sum((mask >> b) & 1 for b in odd_bits(count)) % 2
    return hop(x, mask | turn, count)


def halves(x):
    high = x.astype(BF16)
    return high, (x - high.astype(F32)).astype(BF16)


def add_split(width, shift, a, b, *outs):
    d = digit(shift, width)
    h = outs[0].shape[0]
    for k, out in zip(reversed(range(width)), outs):
        s = pl.ds(flip(d, k, width) * h, h)
        out[...] = a[s] + b[s]


def add_all(*refs):
    vals = [r[...] for r in refs[:-1]]
    while len(vals) > 1:
        vals = [vals[i] + vals[i + 1] for i in range(0, len(vals), 2)]
    refs[-1][...] = vals[0]


def gather(width, shift, *refs):
    d = digit(shift, width)
    out = refs[-1]
    h = refs[0].shape[0]
    for k, r in enumerate(refs[:-1]):
        out[pl.ds(flip(d, k, width) * h, h)] = r[...]


def sum_parts(parts, rest_shift, count):
    width = len(parts)
    piece = (parts[0].shape, F32)
    got = []
    for k in range(1, width):
        got.append(chip_hop(parts[k], 2 * k, count))
    total = call(add_all, [piece], parts[0], *got)[0]
    shift = rest_shift
    while (1 << shift) < count:
        w = min(4, count >> shift)
        got = []
        for k in range(1, w):
            got.append(chip_hop(total, k << shift, count))
        total = call(add_all, [piece], total, *got)[0]
        shift += w.bit_length() - 1
    own = [total]
    for k in range(1, width):
        own.append(chip_hop(total, 2 * k, count))
    half = ((width * piece[0][0],) + piece[0][1:], F32)
    return call(functools.partial(gather, width, 1), [half], *own)[0]


def sum_pair(keep, recv, width, rest_shift, count):
    piece = ((keep.shape[0] // width,) + keep.shape[1:], F32)
    parts = call(functools.partial(add_split, width, 1), [piece] * width, keep, recv)
    return sum_parts(parts[::-1], rest_shift, count)


def start_kernel(tile, step_rows, count, x_hbm, dy_hbm, err_hbm, q_hbm, own, give, keep, send, x_v, xt_v, acc, mix, pt, sem):
    depth = x_v.shape[0]
    rows = own.shape[0]
    cols = dy_hbm.shape[1]
    rank = q_hbm.shape[0]
    c = part_of(count)
    steps = own.shape[1] // tile
    copy = pltpu.make_async_copy(x_hbm, x_v, sem)
    copy.start()
    acc[...] = jnp.zeros_like(acc)
    mix[...] = jnp.zeros_like(mix)

    def body(idx, dy, err, q):
        (j,) = idx.index

        @pl.when(j == 0)
        def _():
            copy.wait()
            xt_v[...] = x_v[...].T

        def part(to):
            at = pl.ds(pl.multiple_of(lax.rem(j, steps) * tile, tile), tile)
            qh, ql = halves(q[...].T)
            right = jnp.concatenate([qh, ql], axis=1)
            for r in range(0, rows, step_rows):
                rs = pl.ds(r, step_rows)
                m = jnp.dot(xt_v[rs, :], dy[...], preferred_element_type=F32)
                to[rs, at] = m + err[rs, :].astype(F32)
            acc[...] += jnp.dot(err[...], right, preferred_element_type=F32)
            mix[...] += jnp.dot(dy[...], right, preferred_element_type=F32)

        pl.when(j // steps == c)(functools.partial(part, own))
        pl.when(j // steps != c)(functools.partial(part, give))

    pltpu.emit_pipeline(
        body,
        grid=(cols // tile,),
        in_specs=[
            pl.BlockSpec((depth, tile), lambda j: (0, j)),
            pl.BlockSpec((rows, tile), lambda j: (0, j)),
            pl.BlockSpec((rank, tile), lambda j: (0, j)),
        ],
        _explicit_indices=True,
    )(dy_hbm, err_hbm, q_hbm)
    uh, ul = halves(mix[:, 0:rank] + mix[:, rank : 2 * rank])
    acc[...] += jnp.dot(xt_v[...], jnp.concatenate([uh, ul], axis=1), preferred_element_type=F32)
    h = keep.shape[0]
    for b in range(rows // LANES):
        a = acc[b * LANES : (b + 1) * LANES, :]
        pt[b] = (a[:, 0:rank] + a[:, rank : 2 * rank]).T
    keep[...] = pt[pl.ds(c * h, h)]
    send[...] = pt[pl.ds((1 - c) * h, h)]


def pair_kernel(tile, own, got, hi, lo):
    def body(j, carry):
        at = pl.ds(pl.multiple_of(j * tile, tile), tile)
        hi[:, at], lo[:, at] = halves(own[:, at] + got[:, at])
        return carry

    lax.fori_loop(0, own.shape[1] // tile, body, 0)


def right_kernel(scale, mine, change, out):
    rank = mine.shape[1]
    q = changed(change, [mine[b] for b in range(mine.shape[0])], scale)
    for b in range(mine.shape[0]):
        qh, ql = halves(q[:, b * LANES : (b + 1) * LANES].T)
        out[b * LANES : (b + 1) * LANES, 0:rank] = qh
        out[b * LANES : (b + 1) * LANES, rank : 2 * rank] = ql


def left_kernel(which, count, hi, lo, right, out):
    rank = right.shape[1] // 2
    h = out.shape[0]
    c = part_of(count)
    first = (c if which == 0 else 1 - c) * h * LANES
    for r in range(0, h * LANES, 256):
        rs = pl.ds(pl.multiple_of(first + r, 256), 256)
        a = jnp.dot(hi[rs, :], right[...], preferred_element_type=F32)
        b = jnp.dot(lo[rs, :], right[:, 0:rank], preferred_element_type=F32)
        p = a[:, 0:rank] + a[:, rank : 2 * rank] + b
        for i in range(256 // LANES):
            out[r // LANES + i] = p[i * LANES : (i + 1) * LANES].T


def basis_kernel(count, mine, other, basis, change):
    p_all = joined(count, mine, other)
    rank, size = p_all.shape
    blocks = size // LANES
    group = 8
    tiles = rank // group
    p = [[p_all[t * group : (t + 1) * group, b * LANES : (b + 1) * LANES] for b in range(blocks)] for t in range(tiles)]
    row_of = lax.broadcasted_iota(jnp.int32, (group, 1), 0)
    lane_of = lax.broadcasted_iota(jnp.int32, (group, LANES), 1)
    unit = [jnp.where(lane_of == row_of + t * group, 1.0, 0.0) for t in range(tiles)]
    v = [row + [u] for row, u in zip(p, unit)]
    for k in range(rank):
        t0, r0 = divmod(k, group)
        vk = [x[r0 : r0 + 1, :] for x in v[t0]]
        sq = functools.reduce(jnp.add, [x * x for x in vk[:blocks]])
        scale = lax.rsqrt(jnp.sum(sq, axis=1, keepdims=True) + 1.0)
        bk = [x * scale for x in vk]
        for t in range(t0, tiles):
            dots = functools.reduce(jnp.add, [p[t][b] * vk[b] for b in range(blocks)])
            coef = jnp.sum(dots, axis=1, keepdims=True) * scale
            if t == t0:
                coef = jnp.where(row_of > r0, coef, 0.0)
                here = row_of == r0
                v[t] = [jnp.where(here, y, x - coef * y) for x, y in zip(v[t], bk)]
            else:
                v[t] = [x - coef * y for x, y in zip(v[t], bk)]
    for t in range(tiles):
        rows = slice(t * group, (t + 1) * group)
        change[rows, :] = v[t][blocks]
        for b in range(blocks):
            basis[rows, b * LANES : (b + 1) * LANES] = v[t][b]


def factor_kernel(count, picks, width, hi, lo, mine, other, *outs):
    rank = mine.shape[1]
    h = outs[0].shape[0]
    d = digit(1, width)
    left = jnp.concatenate(thirds(joined(count, mine, other)), axis=0)
    for k, out in zip(picks, outs):
        at = pl.ds(pl.multiple_of(flip(d, k, width) * (h * LANES), h * LANES), h * LANES)
        a = jnp.dot(left, hi[:, at], preferred_element_type=F32)
        b = jnp.dot(left, lo[:, at], preferred_element_type=F32)
        q = (a[0:rank] + b[0:rank]) + (a[rank : 2 * rank] + b[rank : 2 * rank]) + (a[2 * rank :] + b[2 * rank :])
        for i in range(h):
            out[i] = q[:, i * LANES : (i + 1) * LANES]


def changed(change, blocks, scale):
    rank = blocks[0].shape[0]
    wide = jnp.concatenate(blocks, axis=1) * scale
    return jnp.dot(change[:, 0:rank], wide, precision=lax.Precision.HIGHEST, preferred_element_type=F32)


def end_kernel(scale, tile, count, own, give, basis, change, mine, other, master, err_hbm, q_hbm, master_out, q_v, left_v, right_v, master_v, sem):
    rows, cols = own.shape[0], 2 * own.shape[1]
    steps = own.shape[1] // tile
    rank = basis.shape[0]
    c = part_of(count)
    bh, bl = halves(basis[...].T)
    left_v[...] = jnp.concatenate([bh, bl, bh], axis=1)
    h = mine.shape[0]
    for ref, part in ((mine, c), (other, 1 - c)):
        at = pl.ds(pl.multiple_of(part * h * LANES, h * LANES), h * LANES)
        q_v[:, at] = changed(change, [ref[b] for b in range(h)], scale)
    qh, ql = halves(q_v[...])
    right_v[...] = jnp.concatenate([qh, qh, ql], axis=0)
    width = master.shape[1]
    wide = max(width, LANES)
    begin = lax.axis_index("rep") * width
    at = pl.ds(pl.multiple_of(begin // wide * wide, wide), wide)
    recon = jnp.dot(left_v[...], right_v[:, at], preferred_element_type=F32)
    part = lax.rem(begin, wide) // width
    recon = functools.reduce(
        lambda kept, i: jnp.where(part == i, recon[:, i * width : (i + 1) * width], kept),
        range(1, wide // width),
        recon[:, 0:width],
    )
    master_v[...] = master[...] - 0.5 * recon
    copy = pltpu.make_async_copy(master_v, master_out, sem)
    copy.start()

    def body(idx, err, q):
        (j,) = idx.index
        at = pl.ds(pl.multiple_of(j * tile, tile), tile)
        q[...] = q_v[:, at]

        def part(merged):
            here = pl.ds(pl.multiple_of(lax.rem(j, steps) * tile, tile), tile)
            for r in range(0, rows, 256):
                rs = pl.ds(r, 256)
                rec = jnp.dot(left_v[rs, :], right_v[:, at], preferred_element_type=F32)
                err[rs, :] = (merged[rs, here] - rec).astype(BF16)

        pl.when(j // steps == c)(functools.partial(part, own))
        pl.when(j // steps != c)(functools.partial(part, give))

    pltpu.emit_pipeline(
        body,
        grid=(cols // tile,),
        in_specs=[],
        out_specs=[
            pl.BlockSpec((rows, tile), lambda j: (0, j)),
            pl.BlockSpec((rank, tile), lambda j: (0, j)),
        ],
        _explicit_indices=True,
    )(err_hbm, q_hbm)
    copy.wait()


def shards(inputs, out_grads, error_in, q_start, master):
    count = lax.axis_size("rep")
    depth, rows = inputs.shape
    cols = out_grads.shape[1]
    rank = q_start.shape[0]
    p_blocks, q_blocks = rows // LANES, cols // LANES
    p_half = ((p_blocks // 2, rank, LANES), F32)
    width = min(4, count // 2)
    rest = width.bit_length()
    q_piece = ((q_blocks // 2 // width, rank, LANES), F32)
    half = (rows, cols // 2)
    work = 3 * rows * cols * rank
    tile = 512
    own, give, keep, send = call(
        functools.partial(start_kernel, 2 * tile, rows, count),
        [(half, F32), (half, F32), p_half, p_half],
        inputs,
        out_grads,
        error_in.reshape(rows, cols),
        q_start,
        any_in=(0, 1, 2, 3),
        scratch=[
            pltpu.VMEM((depth, rows), BF16),
            pltpu.VMEM((rows, depth), BF16),
            pltpu.VMEM((rows, 2 * rank), F32),
            pltpu.VMEM((depth, 2 * rank), F32),
            pltpu.VMEM((p_blocks, rank, LANES), F32),
            pltpu.SemaphoreType.DMA,
        ],
        limit=20,
        flops=2 * depth * rows * cols,
    )
    recv, give = lax.optimization_barrier((hop(send, 1, count), give))
    got = hop(give, 1, count)
    for step in range(ITERS):
        mine = sum_pair(keep, recv, width, rest, count)
        other = hop(mine, 1, count)
        left = (mine, other)
        basis, change = call(functools.partial(basis_kernel, count), [((rank, rows), F32), ((rank, LANES), F32)],
                             *left, flops=work)
        if step == 0:
            pair = call(functools.partial(pair_kernel, tile // 2), [(half, BF16), (half, BF16)], own, got,
                        flops=work)
        picks = list(reversed(range(1, width)))
        away = call(functools.partial(factor_kernel, count, picks, width), [q_piece] * len(picks), *pair, *left, flops=work)
        home = call(functools.partial(factor_kernel, count, [0], width), [q_piece], *pair, *left, flops=work)
        mine = sum_parts([*home, *reversed(away)], rest, count)
        if step + 1 < ITERS:
            right = call(functools.partial(right_kernel, 1.0 / count), [((half[1], 2 * rank), BF16)], mine, change)[0]
            send = call(functools.partial(left_kernel, 1, count), [p_half], *pair, right, flops=work)[0]
            recv = hop(send, 1, count)
            keep = call(functools.partial(left_kernel, 0, count), [p_half], *pair, right, flops=work)[0]
    other = hop(mine, 1, count)
    error_out, q_out, master_out = call(
        functools.partial(end_kernel, 1.0 / count, 2 * tile, count),
        [((rows, cols), BF16), ((rank, cols), F32), (master.shape, F32)],
        own, give, basis, change, mine, other, master,
        any_out=(0, 1, 2),
        scratch=[
            pltpu.VMEM((rank, cols), F32),
            pltpu.VMEM((rows, 3 * rank), BF16),
            pltpu.VMEM((3 * rank, cols), BF16),
            pltpu.VMEM(master.shape, F32),
            pltpu.SemaphoreType.DMA,
        ],
        limit=20,
        flops=work,
    )
    return error_out[None], q_out, master_out


def solution(mesh):
    def step(*args):
        with jax.sharding.use_abstract_mesh(mesh.abstract_mesh):
            return jax.shard_map(
                shards,
                mesh=mesh,
                in_specs=(P("rep", None), P("rep", None), P("rep", None, None), P(), P(None, "rep")),
                out_specs=(P("rep", None, None), P(), P(None, "rep")),
                check_vma=False,
            )(*args)

    return step
```

```python
import functools

import jax
import jax.numpy as jnp
from jax import lax
from jax.experimental import pallas as pl
from jax.experimental.pallas import tpu as pltpu
from jax.sharding import PartitionSpec as P


ITERS = 3
LANES = 128
F32 = jnp.float32
BF16 = jnp.bfloat16
VMEM = pl.BlockSpec(memory_space=pltpu.VMEM)
ANY = pl.BlockSpec(memory_space=pltpu.HBM)
MIB = 1 << 20


def call(body, outs, *args, scratch=(), any_in=(), any_out=(), limit=8, flops=0):
    return pl.pallas_call(
        body,
        out_shape=[(pltpu.HBM if i in any_out else pltpu.VMEM)(s, d) for i, (s, d) in enumerate(outs)],
        in_specs=[ANY if i in any_in else VMEM for i in range(len(args))],
        out_specs=[ANY if i in any_out else VMEM for i in range(len(outs))],
        scratch_shapes=list(scratch),
        compiler_params=pltpu.CompilerParams(vmem_limit_bytes=limit * MIB),
        cost_estimate=pl.CostEstimate(flops=flops, bytes_accessed=0, transcendentals=0),
    )(*[pltpu.with_memory_space_constraint(a, pltpu.HBM) if i in any_in else a for i, a in enumerate(args)])


def hop(x, mask, count):
    return lax.ppermute(x, "rep", [(i, i ^ mask) for i in range(count)])


def digit(shift, width):
    return lax.rem(lax.axis_index("rep") // (1 << shift), width)


def flip(value, mask, width):
    out = 0
    bit = 1
    while bit < width:
        b = lax.rem(value // bit, 2)
        out = out + bit * (1 - b if mask & bit else b)
        bit *= 2
    return out


def thirds(x):
    high = x.astype(BF16)
    rest = x - high.astype(F32)
    mid = rest.astype(BF16)
    return [high, mid, (rest - mid.astype(F32)).astype(BF16)]


def joined(count, mine, other):
    c = part_of(count)
    h = mine.shape[0]
    first = [jnp.where(c == 0, mine[b], other[b]) for b in range(h)]
    second = [jnp.where(c == 0, other[b], mine[b]) for b in range(h)]
    return jnp.concatenate(first + second, axis=1)


def odd_bits(count):
    return [b for b in range(1, count.bit_length() - 1) if b == 1 or b % 2 == 0]


def part_of(count):
    me = lax.axis_index("rep")
    return lax.rem(sum((lax.rem(me // (1 << b), 2) for b in odd_bits(count)), lax.rem(me, 2)), 2)


def chip_hop(x, mask, count):
    turn = sum((mask >> b) & 1 for b in odd_bits(count)) % 2
    return hop(x, mask | turn, count)


def halves(x):
    high = x.astype(BF16)
    return high, (x - high.astype(F32)).astype(BF16)


def add_split(width, shift, a, b, *outs):
    d = digit(shift, width)
    h = outs[0].shape[0]
    for k, out in zip(reversed(range(width)), outs):
        s = pl.ds(flip(d, k, width) * h, h)
        out[...] = a[s] + b[s]


def add_all(*refs):
    vals = [r[...] for r in refs[:-1]]
    while len(vals) > 1:
        vals = [vals[i] + vals[i + 1] for i in range(0, len(vals), 2)]
    refs[-1][...] = vals[0]


def gather(width, shift, *refs):
    d = digit(shift, width)
    out = refs[-1]
    h = refs[0].shape[0]
    for k, r in enumerate(refs[:-1]):
        out[pl.ds(flip(d, k, width) * h, h)] = r[...]


def sum_parts(parts, rest_shift, count):
    width = len(parts)
    piece = (parts[0].shape, F32)
    got = []
    for k in range(1, width):
        got.append(chip_hop(parts[k], 2 * k, count))
    total = call(add_all, [piece], parts[0], *got)[0]
    shift = rest_shift
    while (1 << shift) < count:
        w = min(4, count >> shift)
        got = []
        for k in range(1, w):
            got.append(chip_hop(total, k << shift, count))
        total = call(add_all, [piece], total, *got)[0]
        shift += w.bit_length() - 1
    own = [total]
    for k in range(1, width):
        own.append(chip_hop(total, 2 * k, count))
    return own


def whole_half(pieces):
    width = len(pieces)
    half = ((width * pieces[0].shape[0],) + pieces[0].shape[1:], F32)
    return call(functools.partial(gather, width, 1), [half], *pieces)[0]


def sum_pair(keep, recv, width, rest_shift, count):
    piece = ((keep.shape[0] // width,) + keep.shape[1:], F32)
    parts = call(functools.partial(add_split, width, 1), [piece] * width, keep, recv)
    return whole_half(sum_parts(parts[::-1], rest_shift, count))


def start_kernel(tile, step_rows, count, x_hbm, dy_hbm, err_hbm, q_hbm, own, give, keep, send, x_v, xt_v, acc, mix, pt, sem):
    depth = x_v.shape[0]
    rows = own.shape[0]
    cols = dy_hbm.shape[1]
    rank = q_hbm.shape[0]
    c = part_of(count)
    steps = own.shape[1] // tile
    copy = pltpu.make_async_copy(x_hbm, x_v, sem)
    copy.start()
    acc[...] = jnp.zeros_like(acc)
    mix[...] = jnp.zeros_like(mix)

    def body(idx, dy, err, q):
        (j,) = idx.index

        @pl.when(j == 0)
        def _():
            copy.wait()
            xt_v[...] = x_v[...].T

        def part(to):
            at = pl.ds(pl.multiple_of(lax.rem(j, steps) * tile, tile), tile)
            qh, ql = halves(q[...].T)
            right = jnp.concatenate([qh, ql], axis=1)
            for r in range(0, rows, step_rows):
                rs = pl.ds(r, step_rows)
                m = jnp.dot(xt_v[rs, :], dy[...], preferred_element_type=F32)
                to[rs, at] = m + err[rs, :].astype(F32)
            acc[...] += jnp.dot(err[...], right, preferred_element_type=F32)
            mix[...] += jnp.dot(dy[...], right, preferred_element_type=F32)

        pl.when(j // steps == c)(functools.partial(part, own))
        pl.when(j // steps != c)(functools.partial(part, give))

    pltpu.emit_pipeline(
        body,
        grid=(cols // tile,),
        in_specs=[
            pl.BlockSpec((depth, tile), lambda j: (0, j)),
            pl.BlockSpec((rows, tile), lambda j: (0, j)),
            pl.BlockSpec((rank, tile), lambda j: (0, j)),
        ],
        _explicit_indices=True,
    )(dy_hbm, err_hbm, q_hbm)
    uh, ul = halves(mix[:, 0:rank] + mix[:, rank : 2 * rank])
    acc[...] += jnp.dot(xt_v[...], jnp.concatenate([uh, ul], axis=1), preferred_element_type=F32)
    h = keep.shape[0]
    for b in range(rows // LANES):
        a = acc[b * LANES : (b + 1) * LANES, :]
        pt[b] = (a[:, 0:rank] + a[:, rank : 2 * rank]).T
    keep[...] = pt[pl.ds(c * h, h)]
    send[...] = pt[pl.ds((1 - c) * h, h)]


def pair_kernel(tile, own, got, hi, lo):
    def body(j, carry):
        at = pl.ds(pl.multiple_of(j * tile, tile), tile)
        hi[:, at], lo[:, at] = halves(own[:, at] + got[:, at])
        return carry

    lax.fori_loop(0, own.shape[1] // tile, body, 0)


def right_of(blocks, change, scale):
    q = changed(change, blocks, scale)
    both = [jnp.concatenate(halves(q[:, b * LANES : (b + 1) * LANES].T), axis=1) for b in range(len(blocks))]
    return jnp.concatenate(both, axis=0)


def piece_of(partner, width, size):
    return pl.ds(pl.multiple_of(flip(digit(1, width), partner, width) * size, size), size)


def left_part(hi, lo, rows, cols, right):
    rank = right.shape[1] // 2
    a = jnp.dot(hi[rows, cols], right, preferred_element_type=F32)
    b = jnp.dot(lo[rows, cols], right[:, 0:rank], preferred_element_type=F32)
    return a[:, 0:rank] + a[:, rank : 2 * rank] + b


def own_kernel(scale, width, hi, lo, piece, change, out):
    size = piece.shape[0] * LANES
    right = right_of([piece[b] for b in range(piece.shape[0])], change[...], scale)
    for r in range(0, hi.shape[0], 256):
        p = left_part(hi, lo, pl.ds(r, 256), piece_of(0, width, size), right)
        for i in range(256 // LANES):
            out[r // LANES + i] = p[i * LANES : (i + 1) * LANES].T


def right_kernel(scale, *refs):
    *pieces, change, out = refs
    size = out.shape[0] // len(pieces)
    for k, piece in enumerate(pieces):
        out[k * size : (k + 1) * size, :] = right_of([piece[b] for b in range(piece.shape[0])], change[...], scale)


def left_kernel(which, count, width, hi, lo, right, begun, out):
    h = out.shape[0]
    size = right.shape[0] // (width - 1)
    c = part_of(count)
    block = (c if which == 0 else 1 - c) * h
    for r in range(0, h * LANES, 256):
        rows = pl.ds(pl.multiple_of(block * LANES + r, 256), 256)
        p = functools.reduce(
            jnp.add,
            [
                left_part(hi, lo, rows, piece_of(k, width, size), right[(k - 1) * size : k * size, :])
                for k in range(1, width)
            ],
        )
        for i in range(256 // LANES):
            b = r // LANES + i
            out[b] = begun[block + b] + p[i * LANES : (i + 1) * LANES].T


def basis_kernel(count, mine, other, basis, change):
    p_all = joined(count, mine, other)
    rank, size = p_all.shape
    blocks = size // LANES
    group = 8
    tiles = rank // group
    p = [[p_all[t * group : (t + 1) * group, b * LANES : (b + 1) * LANES] for b in range(blocks)] for t in range(tiles)]
    row_of = lax.broadcasted_iota(jnp.int32, (group, 1), 0)
    lane_of = lax.broadcasted_iota(jnp.int32, (group, LANES), 1)
    unit = [jnp.where(lane_of == row_of + t * group, 1.0, 0.0) for t in range(tiles)]
    v = [row + [u] for row, u in zip(p, unit)]
    for k in range(rank):
        t0, r0 = divmod(k, group)
        vk = [x[r0 : r0 + 1, :] for x in v[t0]]
        sq = functools.reduce(jnp.add, [x * x for x in vk[:blocks]])
        scale = lax.rsqrt(jnp.sum(sq, axis=1, keepdims=True) + 1.0)
        bk = [x * scale for x in vk]
        for t in range(t0, tiles):
            dots = functools.reduce(jnp.add, [p[t][b] * vk[b] for b in range(blocks)])
            coef = jnp.sum(dots, axis=1, keepdims=True) * scale
            if t == t0:
                coef = jnp.where(row_of > r0, coef, 0.0)
                here = row_of == r0
                v[t] = [jnp.where(here, y, x - coef * y) for x, y in zip(v[t], bk)]
            else:
                v[t] = [x - coef * y for x, y in zip(v[t], bk)]
    for t in range(tiles):
        rows = slice(t * group, (t + 1) * group)
        change[rows, :] = v[t][blocks]
        for b in range(blocks):
            basis[rows, b * LANES : (b + 1) * LANES] = v[t][b]


def factor_part(left, hi, lo, first, cols):
    rank = left.shape[0] // 3
    rows = pl.ds(pl.multiple_of(first, left.shape[1]), left.shape[1])
    a = jnp.dot(left, hi[rows, cols], preferred_element_type=F32)
    b = jnp.dot(left, lo[rows, cols], preferred_element_type=F32)
    return (a[0:rank] + b[0:rank]) + (a[rank : 2 * rank] + b[rank : 2 * rank]) + (a[2 * rank :] + b[2 * rank :])


def side_by_side(ref):
    return jnp.concatenate([ref[b] for b in range(ref.shape[0])], axis=1)


def begin_kernel(count, tile, hi, lo, mine, out):
    left = jnp.concatenate(thirds(side_by_side(mine)), axis=0)
    for j in range(0, hi.shape[1], tile):
        q = factor_part(left, hi, lo, part_of(count) * left.shape[1], pl.ds(j, tile))
        for i in range(tile // LANES):
            out[j // LANES + i] = q[:, i * LANES : (i + 1) * LANES]


def factor_kernel(count, picks, width, hi, lo, begun, other, *outs):
    h = outs[0].shape[0]
    d = digit(1, width)
    left = jnp.concatenate(thirds(side_by_side(other)), axis=0)
    for k, out in zip(picks, outs):
        q = factor_part(left, hi, lo, (1 - part_of(count)) * left.shape[1], piece_of(k, width, h * LANES))
        for i in range(h):
            out[i] = begun[flip(d, k, width) * h + i] + q[:, i * LANES : (i + 1) * LANES]


def changed(change, blocks, scale):
    rank = blocks[0].shape[0]
    wide = jnp.concatenate(blocks, axis=1) * scale
    return jnp.dot(change[:, 0:rank], wide, precision=lax.Precision.HIGHEST, preferred_element_type=F32)


def ready_kernel(scale, basis, change, mine, left, q, right):
    bh, bl = halves(basis[...].T)
    left[...] = jnp.concatenate([bh, bl, bh], axis=1)
    part = changed(change, [mine[b] for b in range(mine.shape[0])], scale)
    q[...] = part
    qh, ql = halves(part)
    right[...] = jnp.concatenate([qh, qh, ql], axis=0)


def end_kernel(scale, tile, count, own, give, left_v, q_mine, right_mine, change, other, master,
               err_hbm, q_hbm, master_out, q_v, right_v, master_v, sem):
    rows, cols = own.shape[0], 2 * own.shape[1]
    steps = own.shape[1] // tile
    rank = q_mine.shape[0]
    c = part_of(count)
    h = other.shape[0]
    size = h * LANES
    here = pl.ds(pl.multiple_of(c * size, size), size)
    there = pl.ds(pl.multiple_of((1 - c) * size, size), size)
    q_v[:, here] = q_mine[...]
    right_v[:, here] = right_mine[...]
    part = changed(change, [other[b] for b in range(h)], scale)
    q_v[:, there] = part
    qh, ql = halves(part)
    right_v[:, there] = jnp.concatenate([qh, qh, ql], axis=0)
    width = master.shape[1]
    wide = max(width, LANES)
    begin = lax.axis_index("rep") * width
    at = pl.ds(pl.multiple_of(begin // wide * wide, wide), wide)
    recon = jnp.dot(left_v[...], right_v[:, at], preferred_element_type=F32)
    part = lax.rem(begin, wide) // width
    recon = functools.reduce(
        lambda kept, i: jnp.where(part == i, recon[:, i * width : (i + 1) * width], kept),
        range(1, wide // width),
        recon[:, 0:width],
    )
    master_v[...] = master[...] - 0.5 * recon
    copy = pltpu.make_async_copy(master_v, master_out, sem)
    copy.start()

    def body(idx, err, q):
        (j,) = idx.index
        at = pl.ds(pl.multiple_of(j * tile, tile), tile)
        q[...] = q_v[:, at]

        def part(merged):
            here = pl.ds(pl.multiple_of(lax.rem(j, steps) * tile, tile), tile)
            for r in range(0, rows, 256):
                rs = pl.ds(r, 256)
                rec = jnp.dot(left_v[rs, :], right_v[:, at], preferred_element_type=F32)
                err[rs, :] = (merged[rs, here] - rec).astype(BF16)

        pl.when(j // steps == c)(functools.partial(part, own))
        pl.when(j // steps != c)(functools.partial(part, give))

    pltpu.emit_pipeline(
        body,
        grid=(cols // tile,),
        in_specs=[],
        out_specs=[
            pl.BlockSpec((rows, tile), lambda j: (0, j)),
            pl.BlockSpec((rank, tile), lambda j: (0, j)),
        ],
        _explicit_indices=True,
    )(err_hbm, q_hbm)
    copy.wait()


def shards(inputs, out_grads, error_in, q_start, master):
    count = lax.axis_size("rep")
    depth, rows = inputs.shape
    cols = out_grads.shape[1]
    rank = q_start.shape[0]
    p_blocks, q_blocks = rows // LANES, cols // LANES
    p_half = ((p_blocks // 2, rank, LANES), F32)
    width = min(4, count // 2)
    rest = width.bit_length()
    q_piece = ((q_blocks // 2 // width, rank, LANES), F32)
    half = (rows, cols // 2)
    work = 3 * rows * cols * rank
    tile = 512
    own, give, keep, send = call(
        functools.partial(start_kernel, 2 * tile, rows, count),
        [(half, F32), (half, F32), p_half, p_half],
        inputs,
        out_grads,
        error_in.reshape(rows, cols),
        q_start,
        any_in=(0, 1, 2, 3),
        scratch=[
            pltpu.VMEM((depth, rows), BF16),
            pltpu.VMEM((rows, depth), BF16),
            pltpu.VMEM((rows, 2 * rank), F32),
            pltpu.VMEM((depth, 2 * rank), F32),
            pltpu.VMEM((p_blocks, rank, LANES), F32),
            pltpu.SemaphoreType.DMA,
        ],
        limit=20,
        flops=2 * depth * rows * cols,
    )
    recv, give = lax.optimization_barrier((hop(send, 1, count), give))
    got = hop(give, 1, count)
    for step in range(ITERS):
        mine = sum_pair(keep, recv, width, rest, count)
        other = hop(mine, 1, count)
        left = (mine, other)
        basis, change = call(functools.partial(basis_kernel, count), [((rank, rows), F32), ((rank, LANES), F32)],
                             *left, flops=work)
        if step == 0:
            pair = call(functools.partial(pair_kernel, tile // 2), [(half, BF16), (half, BF16)], own, got,
                        flops=work)
        begun = call(functools.partial(begin_kernel, count, tile), [((q_blocks // 2, rank, LANES), F32)], *pair, mine,
                     flops=work)[0]
        picks = list(reversed(range(1, width)))
        away = call(functools.partial(factor_kernel, count, picks, width), [q_piece] * len(picks), *pair, begun, other,
                    flops=work)
        home = call(functools.partial(factor_kernel, count, [0], width), [q_piece], *pair, begun, other, flops=work)
        pieces = sum_parts([*home, *reversed(away)], rest, count)
        if step + 1 < ITERS:
            begun = call(functools.partial(own_kernel, 1.0 / count, width), [((p_blocks, rank, LANES), F32)], *pair,
                         pieces[0], change, flops=work)[0]
            size = (width - 1) * q_piece[0][0] * LANES
            right = call(functools.partial(right_kernel, 1.0 / count), [((size, 2 * rank), BF16)], *pieces[1:], change)[0]
            send = call(functools.partial(left_kernel, 1, count, width), [p_half], *pair, right, begun, flops=work)[0]
            recv = hop(send, 1, count)
            keep = call(functools.partial(left_kernel, 0, count, width), [p_half], *pair, right, begun, flops=work)[0]
    mine = whole_half(pieces)
    other = hop(mine, 1, count)
    left, q_mine, right_mine = call(
        functools.partial(ready_kernel, 1.0 / count),
        [((rows, 3 * rank), BF16), ((rank, half[1]), F32), ((3 * rank, half[1]), BF16)],
        basis, change, mine, flops=work,
    )
    error_out, q_out, master_out = call(
        functools.partial(end_kernel, 1.0 / count, 2 * tile, count),
        [((rows, cols), BF16), ((rank, cols), F32), (master.shape, F32)],
        own, give, left, q_mine, right_mine, change, other, master,
        any_out=(0, 1, 2),
        scratch=[
            pltpu.VMEM((rank, cols), F32),
            pltpu.VMEM((3 * rank, cols), BF16),
            pltpu.VMEM(master.shape, F32),
            pltpu.SemaphoreType.DMA,
        ],
        limit=20,
        flops=work,
    )
    return error_out[None], q_out, master_out


def solution(mesh):
    def step(*args):
        with jax.sharding.use_abstract_mesh(mesh.abstract_mesh):
            return jax.shard_map(
                shards,
                mesh=mesh,
                in_specs=(P("rep", None), P("rep", None), P("rep", None, None), P(), P(None, "rep")),
                out_specs=(P("rep", None, None), P(), P(None, "rep")),
                check_vma=False,
            )(*args)

    return step
```
